32 devices in a mesh: frame: 4 (over x, core), rank: 8 (over z, y).
Axes of the slice: x: 2, y: 2, z: 4, core: 2. Of those that a mesh axis runs over, the one named last changes fastest.
Arguments:
- layers: float32 [4, 8, 4, 32, 16384], P('frame', 'rank')
- depth_order: int32 [4, 8], P('frame'), may hold values from 0 to 7, as said below
- tile_slots: int32 [32], replicated, may hold values from 0 to 31, each once
Outputs:
- filtered: float32 [32, 4, 4, 16384], P('frame', None, None, 'rank')
- coverage: float32 [4], P('frame')
The draws below stay inside these ranges and needn't reach their ends.
Inputs may be any that keep to these rules, and one draw needn't show every extreme that they name: `depth_order`: each row is a permutation of the ranks in which, for every bit b, the ranks that agree on all bits from b upward take consecutive depths. `tile_slots`: slot s belongs to frame group s // 8.
All inputs are finite; a program needn't handle non-finite values.
Results may differ from the reference program's by a relative error of at most 0.00002.
Values sent between devices are 32-bit elements; how exact they have to be, the bound alone decides.
No kernel may reach another device: no remote copies, remote signals or barrier semaphores. Data moves between devices by JAX's collectives and lax.ppermute only.
A program may use at most 64 MiB of HBM per device.

```python
import jax
import jax.numpy as jnp
from jax import lax

TILE = 128
TILES = 32
FRAMES = 4
RANKS = 8


def draw_layers(key, part):
    key_alpha, key_color, key_block = jax.random.split(jax.random.fold_in(key, 11), 3)
    piece_len = TILE * TILE // RANKS
    shape = (FRAMES, RANKS, 1, TILES, RANKS, piece_len)
    alpha = jnp.exp(jax.random.uniform(key_alpha, shape, jnp.float32, jnp.log(0.005), jnp.log(0.08)))
    position = jnp.arange(RANKS, dtype=jnp.float32) / max(RANKS - 1, 1)
    jitter = jax.random.uniform(key_block, (FRAMES, RANKS), jnp.float32, -0.35, 0.35)
    factor = jnp.minimum(jnp.exp(jnp.log(0.12) * (1.0 - position)[None, :] + jitter), 1.0)
    alpha = alpha * factor[:, None, None, None, :, None]
    alpha = alpha.reshape(FRAMES, RANKS, 1, TILES, TILE * TILE)
    color = alpha * jax.random.uniform(key_color, (FRAMES, RANKS, 3, TILES, TILE * TILE), jnp.float32)
    return jnp.concatenate([color, alpha], axis=2).astype(jnp.float32)


def draw_depth_order(key, part):
    levels = RANKS.bit_length() - 1
    ranks = jnp.arange(RANKS, dtype=jnp.int32)
    flips = jax.random.randint(jax.random.fold_in(key, 23), (FRAMES, max(levels, 1), RANKS), 0, 2).astype(jnp.int32)
    place = jnp.broadcast_to(ranks[None, :], (FRAMES, RANKS))
    for level in range(levels):
        parent = ranks >> level + 1
        place = place ^ flips[:, level, parent] << level
    frame_ids = jnp.arange(FRAMES, dtype=jnp.int32)[:, None]
    order = jnp.zeros((FRAMES, RANKS), jnp.int32).at[frame_ids, place].set(jnp.broadcast_to(ranks[None, :], (FRAMES, RANKS)))
    return order


def setup_inputs(seed: int = 0) -> dict:
    key_list = jax.random.split(jax.random.key(seed), 4)
    layers = draw_layers(jax.random.fold_in(key_list[3], 71), 0)
    depth_order = draw_depth_order(jax.random.fold_in(key_list[3], 71), 0)
    tile_slots = jax.random.permutation(key_list[2], TILES).astype(jnp.int32)
    return dict(layers=layers, depth_order=depth_order, tile_slots=tile_slots)


def one_frame(operands):
    frame_layers, order = operands

    def blend(total, rank_id):
        layer = lax.dynamic_index_in_dim(frame_layers, rank_id, 0, keepdims=False)
        return total + (1.0 - total[3:4]) * layer, None

    start = jnp.zeros(frame_layers.shape[1:], jnp.float32)
    total, unused = lax.scan(blend, start, order)
    return total


def reference(layers, depth_order, tile_slots):
    composite = lax.map(one_frame, (layers, depth_order))
    coverage = jnp.sum(composite[:, 3], axis=(1, 2)) / (TILES * TILE * TILE)
    picked = composite[:, :, tile_slots, :]
    before = jnp.concatenate([picked[:1], picked[:-1]], axis=0)
    after = jnp.concatenate([picked[1:], picked[-1:]], axis=0)
    smooth = 0.25 * before + 0.5 * picked + 0.25 * after
    filtered = jnp.transpose(smooth, (2, 0, 1, 3))
    return filtered, coverage
```

```python
import functools

import jax
import jax.numpy as jnp
from jax import lax
from jax.experimental import pallas as pl
from jax.experimental.pallas import tpu as pltpu
from jax.sharding import PartitionSpec as P

LANES = 128
SUBLANES = 8
WEIGHTS = (6, 5, 3, 2)


VMEM = pl.BlockSpec(memory_space=pltpu.VMEM)
SMEM = pl.BlockSpec(memory_space=pltpu.SMEM)
ANY = pl.BlockSpec(memory_space=pl.ANY)


def chunk_bounds(total):
    whole = sum(WEIGHTS)
    edges = [0]
    running = 0
    for weight in WEIGHTS:
        running += weight
        edge = (total * running + whole // 2) // whole
        if edge > edges[-1]:
            edges.append(edge)
    edges[-1] = total
    return [(a, b - a) for a, b in zip(edges, edges[1:])]


def out_struct(shape):
    return pltpu.VMEM(shape, jnp.float32)


def pack_kernel(start, count, flip, meta, layer, out, sem):
    bit = meta[0] ^ flip
    copy = pltpu.make_async_copy(layer.at[:, :, :, bit, pl.ds(start, count)], out, sem)
    copy.start()
    copy.wait()


def pack(meta, layer, start, count, flip):
    channels, groups, half, two, total, sub, lanes = layer.shape
    return pl.pallas_call(
        functools.partial(pack_kernel, start, count, flip),
        out_shape=jax.ShapeDtypeStruct((channels, groups, half, count, sub, lanes), jnp.float32),
        in_specs=[SMEM, ANY],
        out_specs=VMEM,
        scratch_shapes=[pltpu.SemaphoreType.DMA],
        name="pack",
    )(meta, layer)


def over(front, mine, theirs):
    near = [jnp.where(front, a, b) for a, b in zip(mine, theirs)]
    far = [jnp.where(front, b, a) for a, b in zip(mine, theirs)]
    clear = 1.0 - near[-1]
    return [a + clear * b for a, b in zip(near, far)]


def blend_kernel(level, meta, mine, theirs, send, keep):
    channels, groups, half = mine.shape[:3]
    front = meta[2 + 2 * level] > 0
    bit = meta[1 + 2 * (level + 1)]

    def group(g, carry):
        for h in range(half // 2):
            for flip, out in ((1, send), (0, keep)):
                at = 2 * h + (bit ^ flip)
                done = over(
                    front,
                    [mine[c, g, at] for c in range(channels)],
                    [theirs[c, g, at] for c in range(channels)],
                )
                for c in range(channels):
                    out[c, g, h] = done[c]
        return carry

    lax.fori_loop(0, groups, group, 0)


def blend(meta, mine, theirs, level):
    channels, groups, half, count, sub, lanes = mine.shape
    piece = jax.ShapeDtypeStruct((channels, groups, half // 2, count, sub, lanes), jnp.float32)
    return pl.pallas_call(
        functools.partial(blend_kernel, level),
        out_shape=(piece, piece),
        in_specs=[SMEM, VMEM, VMEM],
        out_specs=(VMEM, VMEM),
        name="blend",
    )(meta, mine, theirs)


def last_kernel(level, frames, meta, slots, mine, theirs, *rest):
    outs, opacity, whole = rest[:frames], rest[frames], rest[frames + 1]
    channels, groups, half, count, sub, lanes = mine.shape
    front = meta[2 + 2 * level] > 0

    def group(g, total):
        done = over(
            front,
            [mine[c, g, 0] for c in range(channels)],
            [theirs[c, g, 0] for c in range(channels)],
        )
        for c in range(channels):
            whole[c, g] = done[c].reshape(count * sub, lanes)
        return total + jnp.sum(done[-1], axis=0)

    opacity[...] = lax.fori_loop(0, groups, group, jnp.zeros((sub, lanes), jnp.float32))
    frame = meta[0]
    per_group = outs[0].shape[0]
    for k, out in enumerate(outs):
        base = (frame ^ k) * per_group

        def slot(i, carry):
            tile = slots[base + i]
            g = tile // sub
            s = tile % sub
            for c in range(channels):
                out[i, pl.ds(c, count, stride=channels), :] = whole[c, g, pl.ds(s, count, stride=sub), :]
            return carry

        lax.fori_loop(0, per_group, slot, 0)


def last(meta, slots, mine, theirs, level, frames):
    channels, groups, half, count, sub, lanes = mine.shape
    per_group = groups * sub // frames
    piece = jax.ShapeDtypeStruct((per_group, count * channels, lanes), jnp.float32)
    return pl.pallas_call(
        functools.partial(last_kernel, level, frames),
        out_shape=(piece,) * frames + (jax.ShapeDtypeStruct((sub, lanes), jnp.float32),),
        in_specs=[SMEM, SMEM, VMEM, VMEM],
        out_specs=(VMEM,) * (frames + 1),
        scratch_shapes=[pltpu.VMEM((channels, groups, count * sub, lanes), jnp.float32)],
        name="last",
    )(meta, slots, mine, theirs)


def filter_kernel(frames, chunks, meta, *refs):
    ins, out = refs[:-1], refs[-1]
    frame = meta[0]
    for mine in range(frames):

        @pl.when(frame == mine)
        def _():
            row = 0
            for j in range(chunks):
                pieces = ins[j * frames : (j + 1) * frames]
                rows = pieces[0].shape[1]
                at = pl.ds(row, rows)

                def slot(i, carry):
                    got = [pieces[f ^ mine][i] for f in range(frames)]
                    for f in range(frames):
                        before = got[max(f - 1, 0)]
                        after = got[min(f + 1, frames - 1)]
                        out[i, f, at, :] = 0.25 * before + 0.5 * got[f] + 0.25 * after
                    return carry

                lax.fori_loop(0, pieces[0].shape[0], slot, 0)
                row += rows


def smooth(meta, pieces, frames):
    flat = [p for chunk in pieces for p in chunk]
    per_group, _, lanes = flat[0].shape
    rows = sum(chunk[0].shape[1] for chunk in pieces)
    return pl.pallas_call(
        functools.partial(filter_kernel, frames, len(pieces)),
        out_shape=jax.ShapeDtypeStruct((per_group, frames, rows, lanes), jnp.float32),
        in_specs=[SMEM] + [VMEM] * len(flat),
        out_specs=VMEM,
        name="smooth",
    )(meta, *flat)


def swap(value, axis, mask):
    size = lax.axis_size(axis)
    return lax.ppermute(value, axis, [(i, i ^ mask) for i in range(size)])


def shards(layers, depth_order, tile_slots):
    ranks = lax.axis_size("rank")
    frames = lax.axis_size("frame")
    levels = ranks.bit_length() - 1
    channels, tiles, pixels = layers.shape[2:]
    groups = tiles // SUBLANES
    total = pixels // ranks // LANES
    layer = layers.reshape(channels, groups, SUBLANES, ranks // 2, 2, total, LANES)
    layer = jnp.transpose(layer, (0, 1, 3, 4, 5, 2, 6))

    rank = lax.axis_index("rank").astype(jnp.int32)
    frame = lax.axis_index("frame").astype(jnp.int32)
    order = depth_order[0]
    depths = jnp.arange(ranks, dtype=jnp.int32)
    place = jnp.sum(jnp.where(order == rank, depths, 0))
    meta = [frame]
    for level in range(levels):
        there = jnp.sum(jnp.where(order == (rank ^ (1 << level)), depths, 0))
        meta += [(rank >> level) & 1, (place < there).astype(jnp.int32)]
    meta = jnp.stack(meta)
    bit = (rank & 1).reshape(1)

    bounds = chunk_bounds(total)
    theirs = [swap(pack(bit, layer, a, n, 1), "rank", 1) for a, n in bounds]
    mine = [pack(bit, layer, a, n, 0) for a, n in bounds]
    pieces = []
    opacity = 0.0
    for a, b in zip(mine, theirs):
        for level in range(levels - 1):
            send, a = blend(meta, a, b, level)
            b = swap(send, "rank", 2 << level)
        *outs, part = last(meta, tile_slots, a, b, levels - 1, frames)
        opacity = opacity + part
        pieces.append([outs[0]] + [swap(outs[k], "frame", k) for k in range(1, frames)])
    for level in range(levels):
        opacity = opacity + swap(opacity, "rank", 1 << level)
    coverage = (jnp.sum(opacity) / (tiles * pixels)).reshape(1)
    filtered = smooth(meta, pieces, frames)
    filtered = filtered.reshape(tiles // frames, frames, total, channels, LANES)
    filtered = jnp.transpose(filtered, (0, 1, 3, 2, 4)).reshape(tiles // frames, frames, channels, total * LANES)
    return (filtered, coverage)


def solution(mesh):
    placed = (P("frame", "rank", None, None, None), P("frame", None), P())
    return jax.shard_map(
        shards,
        mesh=mesh,
        in_specs=placed,
        out_specs=(P("frame", None, None, "rank"), P("frame")),
        check_vma=False,
    )
```
